32 devices in a mesh: dp: 8 (over z, y), head: 4 (over x, core).
Axes of the slice: x: 2, y: 2, z: 4, core: 2. Of those that a mesh axis runs over, the one named last changes fastest.
Arguments:
- token_ids: int32 [4096], P(('dp', 'head')), may hold values from 0 to 31999
- lengths: int32 [8], P('dp'), may hold values from 32 to 512, as said below
- offsets: int32 [8], P('dp'), may hold values from 0 to 480, as said below
- time_steps: int32 [8], P('dp'), may hold values from 0 to 255
- noise_input: bfloat16 [4096, 256], P(('dp', 'head')), may hold values from -6 to 6
- embed_table: bfloat16 [32000, 256], P('dp'), may hold values from -6 to 6
- input_weight: bfloat16 [256, 1024], P('dp'), may hold values from -0.375 to 0.375
- first_gain: bfloat16 [1024], P('dp'), may hold values from 0.5 to 1.5
- first_shift: bfloat16 [1024], P('dp'), may hold values from -3 to 3
- joint_weight: bfloat16 [1024, 3072], P('dp'), may hold values from -0.1875 to 0.1875
- output_weight: bfloat16 [1024, 1024], P('dp'), may hold values from -3 to 3
- second_gain: bfloat16 [1024], P('dp'), may hold values from 0.5 to 1.5
- second_shift: bfloat16 [1024], P('dp'), may hold values from -3 to 3
- up_weight: bfloat16 [1024, 4096], P('dp'), may hold values from -0.1875 to 0.1875
- up_bias: bfloat16 [4096], P('dp'), may hold values from -3 to 3
- down_weight: bfloat16 [4096, 1024], P('dp'), may hold values from -0.09375 to 0.09375
- down_bias: bfloat16 [1024], P('dp'), may hold values from -3 to 3
- time_gain: bfloat16 [256, 1024], P('dp'), may hold values from 0.25 to 1.75
- cotangent: bfloat16 [4096, 1024], P(('dp', 'head')), may hold values from -6 to 6
Outputs:
- layer_out: float32 [4096, 1024], P(('dp', 'head'))
- noise_grad: float32 [4096, 256], P(('dp', 'head'))
- table_grad: float32 [32000, 256], P('dp')
- input_weight_grad: float32 [256, 1024], P('dp')
- first_gain_grad: float32 [1024], P('dp')
- first_shift_grad: float32 [1024], P('dp')
- joint_weight_grad: float32 [1024, 3072], P('dp')
- output_weight_grad: float32 [1024, 1024], P('dp')
- second_gain_grad: float32 [1024], P('dp')
- second_shift_grad: float32 [1024], P('dp')
- up_weight_grad: float32 [1024, 4096], P('dp')
- up_bias_grad: float32 [4096], P('dp')
- down_weight_grad: float32 [4096, 1024], P('dp')
- down_bias_grad: float32 [1024], P('dp')
- time_gain_grad: float32 [256, 1024], P('dp')
The draws below stay inside these ranges and needn't reach their ends.
Inputs may be any that keep to these rules, and one draw needn't show every extreme that they name: `lengths`: every length lies between 32 and 512; one sequence has exactly 512 tokens and one exactly 32. Sequence b occupies the slots b * 512 + offsets[b] up to, not including, b * 512 + offsets[b] + lengths[b]; offsets[b] + lengths[b] <= 512.
All inputs are finite; a program needn't handle non-finite values.
Results may differ from the reference program's by a relative error of at most 0.018.
Values may be sent and summed in bfloat16 or wider, within the bound.
A program may use at most 256 MiB of HBM per device.

```python
import math
import jax
import jax.numpy as jnp
import numpy as np
from jax import lax

D = 1024
HEADS = 16
HSIZE = 64
FF = 4096
EMB = 256
VOCAB = 32000
TIMES = 256
MINLEN = 32
SEQ_MAX = 512
TOKENS = 4096
NSEQ = 8


def sequence_layout(key):
    lengths = jax.random.randint(jax.random.fold_in(key, 11), (NSEQ,), MINLEN, SEQ_MAX + 1)
    picked = jax.random.permutation(jax.random.fold_in(key, 12), NSEQ)
    lengths = lengths.at[picked[0]].set(SEQ_MAX).at[picked[1]].set(MINLEN)
    free_room = SEQ_MAX - lengths + 1
    spread = jax.random.randint(jax.random.fold_in(key, 13), (NSEQ,), 0, 1 << 20)
    offsets = spread % free_room
    offsets = offsets.at[picked[1]].set(SEQ_MAX - MINLEN)
    return (lengths.astype(jnp.int32), offsets.astype(jnp.int32))


def draw_lengths(key, part):
    return sequence_layout(key)[0]


def draw_offsets(key, part):
    return sequence_layout(key)[1]


def touch_ends(entries, rng, smallest, largest):
    longest = entries.shape.index(max(entries.shape))
    spots = []
    for shift in (0, 1):
        where = [jax.random.randint(jax.random.fold_in(rng, axis), (), 0, length) for axis, length in enumerate(entries.shape)]
        where[longest] = (where[longest] + shift) % entries.shape[longest]
        spots.append(tuple(where))
    return entries.at[spots[0]].set(smallest).at[spots[1]].set(largest)


def level_of(rng, shape, cuts, smallest, largest):
    loudness = 1.0
    for axis_at, shards_of in cuts:
        steps = jax.random.uniform(jax.random.fold_in(jax.random.fold_in(rng, 6), axis_at), (shards_of,), jnp.float32, smallest / len(cuts), largest / len(cuts))
        loudness = loudness * jnp.repeat(jnp.exp(steps), shape[axis_at] // shards_of).reshape((-1,) + (1,) * (len(shape) - 1 - axis_at))
    return loudness


def cumulative_ranks(count, skew):
    portions = [(1 << 20) // math.isqrt(rank ** skew) + 1 for rank in range(1, count + 1)]
    width = 1 + sum(portions) // (1 << 30)
    return np.cumsum(np.array([max(1, weight // width) for weight in portions]))


def skewed_ids(stream_key, shape, number_of, slope):
    grid = cumulative_ranks(number_of, slope)
    ticket = jax.random.randint(jax.random.fold_in(stream_key, 1), shape, 0, int(grid[number_of - 1]))
    standing = jnp.searchsorted(jnp.asarray(grid, jnp.int32), ticket, side="right")
    return jax.random.permutation(jax.random.fold_in(stream_key, 2), number_of)[standing].astype(jnp.int32)


def scatter_about(stream_key, shape, deviation, reach, pieces=(), kind=jnp.bfloat16):
    drawn = deviation * jax.random.normal(stream_key, shape, jnp.float32)
    if pieces:
        drawn = drawn * level_of(stream_key, shape, pieces, -0.22, 0.18)
    return jnp.clip(drawn, -reach, reach).astype(kind)


def setup_inputs(seed: int = 0) -> dict:
    arg_keys = jax.random.split(jax.random.key(seed), 20)
    token_ids = touch_ends(skewed_ids(arg_keys[0], (TOKENS,), VOCAB, 2), jax.random.fold_in(arg_keys[0], 3), 0, VOCAB - 1).astype(jnp.int32)
    lengths = draw_lengths(jax.random.fold_in(arg_keys[19], 71), 0)
    offsets = draw_offsets(jax.random.fold_in(arg_keys[19], 71), 0)
    time_steps = touch_ends(jax.random.randint(arg_keys[3], (NSEQ,), 0, TIMES), jax.random.fold_in(arg_keys[3], 1), 0, TIMES - 1).astype(jnp.int32)
    noise_input = scatter_about(arg_keys[4], (TOKENS, EMB), 1.0, 6.0, ((0, 32),))
    embed_table = scatter_about(arg_keys[5], (VOCAB, EMB), 1.0, 6.0, ((0, 8),))
    input_weight = scatter_about(arg_keys[6], (EMB, D), EMB ** -0.5, 0.375, ((0, 8),))
    first_gain = jnp.clip(1.0 + 0.1 * jax.random.normal(arg_keys[7], (D,), jnp.float32), 0.5, 1.5).astype(jnp.bfloat16)
    first_shift = scatter_about(arg_keys[8], (D,), 0.5, 3.0, ((0, 8),))
    joint_weight = scatter_about(arg_keys[9], (D, 3 * D), D ** -0.5, 0.1875, ((0, 8),))
    output_weight = scatter_about(arg_keys[10], (D, D), (D // 256) ** -0.5, 3.0, ((0, 8),))
    second_gain = jnp.clip(1.0 + 0.1 * jax.random.normal(arg_keys[11], (D,), jnp.float32), 0.5, 1.5).astype(jnp.bfloat16)
    second_shift = scatter_about(arg_keys[12], (D,), 0.5, 3.0, ((0, 8),))
    up_weight = scatter_about(arg_keys[13], (D, FF), D ** -0.5, 0.1875, ((0, 8),))
    up_bias = scatter_about(arg_keys[14], (FF,), 0.5, 3.0, ((0, 8),))
    down_weight = scatter_about(arg_keys[15], (FF, D), FF ** -0.5, 0.09375, ((0, 8),))
    down_bias = scatter_about(arg_keys[16], (D,), 0.5, 3.0, ((0, 8),))
    time_gain = jnp.clip(1.0 + 0.15 * jax.random.normal(arg_keys[17], (TIMES, D), jnp.float32), 0.25, 1.75).astype(jnp.bfloat16)
    cotangent = scatter_about(arg_keys[18], (TOKENS, D), 1.0, 6.0, ((0, 32),))
    return {"token_ids": token_ids, "lengths": lengths, "offsets": offsets, "time_steps": time_steps, "noise_input": noise_input, "embed_table": embed_table, "input_weight": input_weight, "first_gain": first_gain, "first_shift": first_shift, "joint_weight": joint_weight, "output_weight": output_weight, "second_gain": second_gain, "second_shift": second_shift, "up_weight": up_weight, "up_bias": up_bias, "down_weight": down_weight, "down_bias": down_bias, "time_gain": time_gain, "cotangent": cotangent}


@jax.custom_vjp
def low(v):
    return lax.optimization_barrier(v.astype(jnp.bfloat16)).astype(jnp.float32)

@jax.custom_vjp
def low_back(v):
    return v

def low_keep(v):
    return (low(v), None)

def low_pass(kept, grad):
    return (grad,)

def back_keep(v):
    return (v, None)

def back_low(kept, grad):
    return (low(grad),)
low.defvjp(low_keep, low_pass)
low_back.defvjp(back_keep, back_low)
SIG_LO = 0.5
SIG_HI = 4.0
EPS = 1e-05
ROT_BASE = 10000.0
MASKED = -1e+30
HIGHEST = lax.Precision.HIGHEST

def round_both(values):
    return low_back(low(values))

def layer_norm(values, gain, shift):
    average = lax.optimization_barrier(jnp.mean(values, axis=-1, keepdims=True))
    center = values - average
    inv_std = lax.rsqrt(lax.optimization_barrier(jnp.mean(center * center, axis=-1, keepdims=True)) + EPS)
    return center * inv_std * gain + shift

def rotate(values, positions, sign):
    half_size = values.shape[-1] // 2
    freqs = jnp.exp(-math.log(ROT_BASE) * jnp.arange(half_size, dtype=positions.dtype) / half_size)
    angle = positions[:, None] * freqs[None, :]
    cosine = jnp.cos(angle)[:, None, :]
    sine = sign * jnp.sin(angle)[:, None, :]
    first = values[..., :half_size]
    second = values[..., half_size:]
    return jnp.concatenate([first * cosine - second * sine, second * cosine + first * sine], axis=-1)

def attend(queries, key_rows, value_rows, live_mask):
    raw_scores = jnp.einsum('qhd,khd->hqk', queries, key_rows, precision=HIGHEST) * HSIZE ** (-0.5)
    scores = low_back(raw_scores)
    block_rows = live_mask.shape[0]
    diagonal = jnp.arange(block_rows)[:, None] == jnp.arange(block_rows)[None, :]
    allowed = jnp.logical_or(live_mask[:, None] * live_mask[None, :] > 0.5, diagonal)
    scores = jnp.where(allowed[None], scores, MASKED)
    soft_probs = low(jax.nn.softmax(scores, axis=-1))
    return jnp.einsum('hqk,khd->qhd', soft_probs, value_rows, precision=HIGHEST)
attend_saved = jax.checkpoint(attend)

def attend_one(parts):
    return attend_saved(parts[0], parts[1], parts[2], parts[3])

def normalize(table_rows):
    return low(table_rows * lax.rsqrt(lax.optimization_barrier(jnp.mean(table_rows * table_rows, axis=1, keepdims=True)) + EPS))

def forward(params, unit_table, noise_rows, id_rows, noise_level, time_rows, live_mask, positions):
    w_input, gain_one, shift_one, w_joint, w_output, gain_two, shift_two, w_up, b_up, w_down, b_down, t_gain = params
    row_count = id_rows.shape[0]
    embedded = jnp.take(unit_table, id_rows, axis=0)
    in_scale = lax.rsqrt(1.0 + noise_level * noise_level)
    scaled_input = low(in_scale[:, None] * (embedded + noise_level[:, None] * noise_rows))
    stream_in = low_back(jnp.dot(scaled_input, w_input, precision=HIGHEST))
    normed_one = low(layer_norm(stream_in, gain_one, shift_one))
    joint_act = low_back(jnp.dot(normed_one, w_joint, precision=HIGHEST)).reshape(row_count, 3, HEADS, HSIZE)
    queries = round_both(rotate(joint_act[:, 0], positions, 1.0))
    key_rows = round_both(rotate(joint_act[:, 1], positions, 1.0))
    value_rows = round_both(joint_act[:, 2])
    seq_count = row_count // SEQ_MAX
    block_shape = (seq_count, SEQ_MAX, HEADS, HSIZE)
    attended = lax.map(attend_one, (queries.reshape(block_shape), key_rows.reshape(block_shape), value_rows.reshape(block_shape), live_mask.reshape(seq_count, SEQ_MAX)))
    attended = round_both(attended.reshape(row_count, D))
    stream_mid = stream_in + low_back(jnp.dot(attended, w_output, precision=HIGHEST))
    normed_two = low(layer_norm(stream_mid, gain_two, shift_two))
    up_act = low_back(jnp.dot(normed_two, w_up, precision=HIGHEST)) + b_up
    gelu_out = low(jax.nn.gelu(up_act, approximate=False))
    stream_out = stream_mid + low_back(jnp.dot(gelu_out, w_down, precision=HIGHEST)) + b_down
    out_scale = live_mask[:, None] * jnp.take(t_gain, time_rows, axis=0)
    return out_scale * stream_out

def reference(token_ids, lengths, offsets, time_steps, noise_input, embed_table, input_weight, first_gain, first_shift, joint_weight, output_weight, second_gain, second_shift, up_weight, up_bias, down_weight, down_bias, time_gain, cotangent):
    params = tuple((item.astype(jnp.float32) for item in (input_weight, first_gain, first_shift, joint_weight, output_weight, second_gain, second_shift, up_weight, up_bias, down_weight, down_bias, time_gain)))
    unit_table, table_pull = jax.vjp(normalize, embed_table.astype(jnp.float32))
    slots = jnp.arange(TOKENS, dtype=jnp.int32)
    seq_index = (slots // SEQ_MAX).astype(jnp.int32)
    slot_place = slots % SEQ_MAX
    seq_start = jnp.take(offsets, seq_index)
    extent = jnp.take(lengths, seq_index)
    live_mask = jnp.logical_and(slot_place >= seq_start, slot_place < seq_start + extent).astype(jnp.float32)
    positions = (slot_place - seq_start).astype(jnp.float32)
    time_rows = jnp.take(time_steps, seq_index)
    noise_level = jnp.exp(math.log(SIG_LO) + time_rows.astype(jnp.float32) * (math.log(SIG_HI / SIG_LO) / (TIMES - 1)))
    block_len = SEQ_MAX * math.gcd(NSEQ, max(1, 4096 // SEQ_MAX))
    blocks = TOKENS // block_len

    def by_block(values):
        return values.reshape((blocks, block_len) + values.shape[1:])
    items = (by_block(token_ids), by_block(noise_input.astype(jnp.float32)), by_block(noise_level), by_block(time_rows), by_block(live_mask), by_block(positions), by_block(cotangent.astype(jnp.float32)))

    def scan_step(running, block_item):
        id_rows, noise_rows, level_rows, step_rows, live_rows, place_rows, cot_rows = block_item

        def local_forward(param_set, table_set, noise_set):
            return forward(param_set, table_set, noise_set, id_rows, level_rows, step_rows, live_rows, place_rows)
        out_rows, pullback = jax.vjp(local_forward, params, unit_table, noise_rows)
        grad_params, grad_table, grad_noise = pullback(cot_rows)
        running = (jax.tree.map(lambda a, b: a + b, running[0], grad_params), running[1] + grad_table)
        return (running, (out_rows, grad_noise))
    start_sums = (jax.tree.map(jnp.zeros_like, params), jnp.zeros_like(unit_table))
    (grad_params, grad_unit), (out_rows, noise_rows) = lax.scan(scan_step, start_sums, items)
    table_grad, = table_pull(grad_unit)
    g_input, g_gain_one, g_shift_one, g_joint, g_output, g_gain_two, g_shift_two, g_up, g_up_bias, g_down, g_down_bias, g_time = grad_params
    return (out_rows.reshape(TOKENS, D), noise_rows.reshape(TOKENS, EMB), table_grad, g_input, g_gain_one, g_shift_one, g_joint, g_output, g_gain_two, g_shift_two, g_up, g_up_bias, g_down, g_down_bias, g_time)
```

```python
import functools
import math

import jax
import jax.numpy as jnp
from jax import lax
from jax.experimental import pallas as pl
from jax.experimental.pallas import tpu as pltpu
from jax.sharding import PartitionSpec as P

D = 1024
HEADS = 16
HSIZE = 64
FF = 4096
EMB = 256
VOCAB = 32000
TIMES = 256
SIG_LO = 0.5
SIG_HI = 4.0
EPS = 1e-05
ROT_BASE = 10000.0
MASKED = -1e30

BF = jnp.bfloat16
F32 = jnp.float32


def mm(a, b, dims=((1,), (0,))):
    return lax.dot_general(a, b, (dims, ((), ())), preferred_element_type=F32)


def rotate(values, cosine, sine):
    half = HSIZE // 2
    v = values.reshape(values.shape[0], -1, HSIZE)
    a, b = v[..., :half], v[..., half:]
    out = jnp.concatenate(
        [a * cosine - b * sine, b * cosine + a * sine], axis=-1
    )
    return out.reshape(values.shape)


def norm_parts(values):
    center = values - jnp.mean(values, axis=-1, keepdims=True)
    inv = lax.rsqrt(jnp.mean(center * center, axis=-1, keepdims=True) + EPS)
    return center * inv, inv


def norm_back(grad, hat, inv, gain):
    e = grad * gain
    back = inv * (
        e
        - jnp.mean(e, axis=-1, keepdims=True)
        - hat * jnp.mean(e * hat, axis=-1, keepdims=True)
    )
    return back, jnp.sum(grad * hat, axis=0), jnp.sum(grad, axis=0)


MESH = pl.DeviceIdType.MESH
VM = pl.BlockSpec(memory_space=pltpu.VMEM)
HB = pl.BlockSpec(memory_space=pl.ANY)


class Net:
    def __init__(self, nd, nh, sends, recvs):
        self.nd, self.nh, self.nx = nd, nh, nh // 2
        self.sends, self.recvs, self.count = sends, recvs, 0
        self.d, self.h = lax.axis_index("dp"), lax.axis_index("head")
        self.x, self.c = self.h // 2, self.h % 2
        y = self.d % 2
        z = self.d // 2
        self.p = z + y * (nd - 1 - 2 * z)
        self.pending = []

    def at(self, p):
        p = (p + 2 * self.nd) % self.nd
        y = p // (self.nd // 2)
        z = p + y * (self.nd - 1 - 2 * p)
        return z * 2 + y

    def other_chip(self, k):
        return ((self.x + k) % self.nx) * 2 + self.c

    def partner(self):
        return self.x * 2 + 1 - self.c

    def barrier(self, ring=False, dp_all=False, head=False):
        sem = pltpu.get_barrier_semaphore()
        total = 0
        peers = []
        if dp_all:
            peers += [{"dp": (self.d + k) % self.nd} for k in range(1, self.nd)]
        elif ring:
            peers += [{"dp": self.at(self.p + 1)}, {"dp": self.at(self.p - 1)}]
        if head:
            peers += [{"head": self.partner()}]
            peers += [{"head": self.other_chip(k)} for k in range(1, self.nx)]
        for peer in peers:
            pl.semaphore_signal(sem, inc=1, device_id=peer, device_id_type=MESH)
            total += 1
        pl.semaphore_wait(sem, total)

    def send(self, source, target, peer, slot):
        copy = pltpu.make_async_remote_copy(
            src_ref=source,
            dst_ref=target,
            send_sem=self.sends.at[slot],
            recv_sem=self.recvs.at[slot],
            device_id=peer,
            device_id_type=MESH,
        )
        copy.start()
        self.pending.append(copy)
        return copy

    def slots(self, n):
        first = self.count
        self.count += n
        return first

    def finish(self):
        for copy in self.pending:
            copy.wait_send()


def run(*streams):
    live = list(streams)
    while live:
        for stream in list(live):
            if next(stream, "end") == "end":
                live.remove(stream)


def halves(ref):
    n, w = ref.shape[-2], ref.shape[-1]
    if n % 32 == 0:
        return ref.at[pl.ds(0, n // 2)], ref.at[pl.ds(n // 2, n // 2)]
    if w % 256 == 0:
        return ref.at[:, pl.ds(0, w // 2)], ref.at[:, pl.ds(w // 2, w // 2)]
    return ref, None


def ring_gather(net, buf):
    half = net.nd // 2
    first = net.slots(2 * half)
    right, left = {"dp": net.at(net.p + 1)}, {"dp": net.at(net.p - 1)}
    came = []
    for s in range(half):
        for copy in came:
            copy.wait_recv()
        onward, back = buf.at[net.at(net.p - s)], buf.at[net.at(net.p + s)]
        if s == half - 1:
            onward, back = halves(onward)[0], halves(back)[1]
        came = [net.send(onward, onward, right, first + 2 * s)]
        if back is not None:
            came.append(net.send(back, back, left, first + 2 * s + 1))
        yield
    for copy in came:
        copy.wait_recv()


def add_into(ref, other):
    ref[...] = (ref[...].astype(F32) + other[...].astype(F32)).astype(ref.dtype)


def ring_reduce(net, terms, fwd, bwd, out):
    half = net.nd // 2
    first = net.slots(2 * half)
    right, left = {"dp": net.at(net.p + 1)}, {"dp": net.at(net.p - 1)}
    a, b = halves(terms.at[net.at(net.p + half)])
    ta, tb = halves(fwd.at[0])[0], halves(bwd.at[0])[1]
    came = [net.send(a, ta, right, first)]
    if b is not None:
        came.append(net.send(b, tb, left, first + 1))
    yield
    for s in range(1, half):
        for copy in came:
            copy.wait_recv()
        own_f, own_b = terms.at[net.at(net.p + half - s)], terms.at[net.at(net.p - half + s)]
        if s == 1:
            (of, of2), (ob2, ob) = halves(own_f), halves(own_b)
            (ff, ff2), (bb2, bb) = halves(fwd.at[0]), halves(bwd.at[0])
            add_into(ff, of)
            if of2 is not None:
                ff2[...] = of2[...]
                add_into(bb, ob)
                bb2[...] = ob2[...]
            else:
                bwd[0] = own_b[...]
        else:
            add_into(fwd.at[s - 1], own_f)
            add_into(bwd.at[s - 1], own_b)
        came = [
            net.send(fwd.at[s - 1], fwd.at[s], right, first + 2 * s),
            net.send(bwd.at[s - 1], bwd.at[s], left, first + 2 * s + 1),
        ]
        yield
    for copy in came:
        copy.wait_recv()
    total = fwd[half - 1].astype(F32) + bwd[half - 1].astype(F32)
    out[...] = (total + terms[net.d].astype(F32)).astype(out.dtype)


def head_gather(net, buf):
    nx = net.nx
    first = net.slots(2 * nx)
    mate = {"head": net.partner()}
    own = buf.at[net.h]
    far = [
        net.send(own, own, {"head": net.other_chip(k)}, first + k) for k in range(1, nx)
    ]
    near = [net.send(own, own, mate, first)]
    yield
    for k in range(1, nx):
        far[k - 1].wait_recv()
        block = buf.at[net.other_chip(nx - k)]
        near.append(net.send(block, block, mate, first + nx + k))
    yield
    for copy in near:
        copy.wait_recv()


def head_reduce(net, terms, mine, sums, theirs, out):
    nx = net.nx
    first = net.slots(2 * nx)
    mate = {"head": net.partner()}
    order = list(range(1, nx)) + [0]
    near = {}
    for k in order:
        x = (net.x + k) % nx
        near[k] = net.send(terms.at[x * 2 + 1 - net.c], mine.at[x], mate, first + k)
    yield
    far = []
    for k in order:
        x = (net.x + k) % nx
        near[k].wait_recv()
        if k:
            sums[k] = (
                terms[x * 2 + net.c].astype(F32) + mine[x].astype(F32)
            ).astype(sums.dtype)
            peer = {"head": x * 2 + net.c}
            far.append(net.send(sums.at[k], theirs.at[net.x], peer, first + nx + k))
    yield
    total = terms[net.h].astype(F32) + mine[net.x].astype(F32)
    for k in range(1, nx):
        far[k - 1].wait_recv()
        total = total + theirs[(net.x + nx - k) % nx].astype(F32)
    out[...] = total.astype(out.dtype)


def dp_exchange(net, parts, slots):
    nd = net.nd
    first = net.slots(nd)
    came = [
        net.send(
            parts.at[(net.d + k) % nd],
            slots.at[net.d],
            {"dp": (net.d + k) % nd},
            first + k,
        )
        for k in range(1, nd)
    ]
    yield
    for copy in came:
        copy.wait_recv()


def call(body, nd, nh, ident, outs, ins, scratch=(), sems=8, specs=None, out_specs=None):
    def kernel(*refs):
        net = Net(nd, nh, refs[-2], refs[-1])
        body(net, *refs[:-2])
        net.finish()

    return pl.pallas_call(
        kernel,
        out_shape=[jax.ShapeDtypeStruct(*o) for o in outs],
        in_specs=specs or [VM] * len(ins),
        out_specs=out_specs or [VM] * len(outs),
        scratch_shapes=list(scratch)
        + [pltpu.SemaphoreType.DMA((sems,)), pltpu.SemaphoreType.DMA((sems,))],
        compiler_params=pltpu.CompilerParams(
            collective_id=ident, has_side_effects=True
        ),
    )(*ins)


def ids_body(net, ints, out):
    out[net.h, net.d] = ints[...]
    net.barrier(dp_all=True, head=True)
    first = net.slots(net.nd)
    own = out.at[net.h, net.d]
    came = [
        net.send(own, own, {"dp": (net.d + k) % net.nd}, first + k)
        for k in range(1, net.nd)
    ]
    for copy in came:
        copy.wait_recv()
    run(head_gather(net, out))


def gather_body(net, *refs):
    (parts, noise, scal, cot, small_in, in_in, joint_in, out_in, up_in, down_in) = refs[:10]
    (scaled, seq_gain, cots, small, in_w, joint, outs, up, down) = refs[10:19]
    slots = refs[19]
    d, h = net.d, net.h
    small[d] = small_in[...]
    in_w[d] = in_in[...]
    joint[d] = joint_in[...]
    outs[h, d] = out_in[...]
    up[d] = up_in[...]
    down[d] = down_in[...]
    cots[h] = cot[...]
    slots[d] = parts[d]
    net.barrier(dp_all=True, head=True)

    def embed():
        yield from dp_exchange(net, parts, slots)
        rows = noise.shape[0]
        total = slots[0].astype(F32)
        for k in range(1, net.nd):
            total = total + slots[k].astype(F32)
        seq_gain[...] = total[rows:]
        value = scal[0:1] * (total[:rows] + scal[1:2] * noise[...].astype(F32))
        scaled[h] = value.astype(BF)
        yield
        yield from head_gather(net, scaled)
        yield from head_gather(net, cots)

    def outer():
        yield from ring_gather(net, outs.at[h])
        yield from head_gather(net, outs)

    run(
        embed(),
        ring_gather(net, in_w),
        ring_gather(net, small),
        ring_gather(net, joint),
        outer(),
        ring_gather(net, up),
        ring_gather(net, down),
    )


def head_gather_body(net, own, out):
    out[net.h] = own[...]
    net.barrier(head=True)
    run(head_gather(net, out))


def head_reduce_body(net, count, *refs):
    terms, outs = refs[:count], refs[count : 2 * count]
    mine, sums, theirs = [refs[(2 + i) * count : (3 + i) * count] for i in range(3)]
    net.barrier(head=True)
    run(
        *[
            head_reduce(net, terms[i], mine[i], sums[i], theirs[i], outs[i])
            for i in range(count)
        ]
    )


def final_body(net, count, *refs):
    terms = refs[:count]
    emb_in, seq_in = refs[count : count + 2]
    outs = refs[count + 2 : 2 * count + 2]
    emb, seq = refs[2 * count + 2 : 2 * count + 4]
    fwd = refs[2 * count + 4 : 3 * count + 4]
    bwd = refs[3 * count + 4 : 4 * count + 4]
    h, d = net.h, net.d
    emb[h, d] = emb_in[...]
    seq[h, d] = seq_in[...]
    net.barrier(ring=True, head=True)

    def both(ref):
        yield from ring_gather(net, ref.at[h])
        yield from head_gather(net, ref)

    def total(i):
        yield from ring_reduce(net, terms[i], fwd[i], bwd[i], outs[i].at[h])
        yield from head_gather(net, outs[i])

    run(both(emb), both(seq), *[total(i) for i in range(count)])


def per_device(
    token_ids,
    lengths,
    offsets,
    time_steps,
    noise_input,
    embed_table,
    input_weight,
    first_gain,
    first_shift,
    joint_weight,
    output_weight,
    second_gain,
    second_shift,
    up_weight,
    up_bias,
    down_weight,
    down_bias,
    time_gain,
    cotangent,
):
    nd, nh = lax.axis_size("dp"), lax.axis_size("head")
    di, hi = lax.axis_index("dp"), lax.axis_index("head")
    rows = token_ids.shape[0]
    group = rows * nh
    lh = HEADS // nh
    lc = lh * HSIZE
    sub = FF // (nd * nh)
    vrows = embed_table.shape[0]
    trows = time_gain.shape[0]

    slot = jnp.arange(group, dtype=jnp.int32)
    live = jnp.logical_and(slot >= offsets[0], slot < offsets[0] + lengths[0])
    livef = live.astype(F32)
    position = (slot - offsets[0]).astype(F32)
    level = jnp.exp(
        math.log(SIG_LO)
        + time_steps[0].astype(F32) * (math.log(SIG_HI / SIG_LO) / (TIMES - 1))
    )
    in_scale = lax.rsqrt(1.0 + level * level)
    freqs = jnp.exp(
        -math.log(ROT_BASE) * jnp.arange(HSIZE // 2, dtype=F32) / (HSIZE // 2)
    )
    angle = position[:, None] * freqs[None, :]
    cosine = jnp.cos(angle)[:, None, :]
    sine = jnp.sin(angle)[:, None, :]

    def own(x):
        return lax.dynamic_slice_in_dim(x, hi * rows, rows, 0)

    link = functools.partial(call, nd=nd, nh=nh)
    ints = jnp.concatenate(
        [
            token_ids[None],
            jnp.broadcast_to(time_steps[:, None], (1, rows)),
            jnp.zeros((6, rows), jnp.int32),
        ]
    )
    (ints_all,) = link(
        ids_body,
        ident=0,
        outs=[((nh, nd, 8, rows), jnp.int32)],
        ins=[ints],
        sems=nd + 2 * nh,
    )
    ids_dp = lax.dynamic_index_in_dim(ints_all, hi, 0, False)[:, 0].reshape(-1)
    times_all = ints_all[0, :, 1, 0]
    table_f = embed_table.astype(F32)
    table_inv = lax.rsqrt(jnp.mean(table_f * table_f, axis=1, keepdims=True) + EPS)
    unit = (table_f * table_inv).astype(BF)
    vocab_iota = jnp.arange(vrows, dtype=jnp.int32) + di * vrows
    pick = (ids_dp[:, None] == vocab_iota[None, :]).astype(BF)
    time_iota = jnp.arange(trows, dtype=jnp.int32) + di * trows
    time_pick = (times_all[:, None] == time_iota[None, :]).astype(BF)
    time_rows = mm(time_pick, time_gain).astype(BF).reshape(nd, D // EMB, EMB)
    parts = jnp.concatenate(
        [
            mm(pick, unit).astype(BF).reshape(nd, rows, EMB),
            time_rows,
            jnp.zeros((nd, 16 - D // EMB, EMB), BF),
        ],
        axis=1,
    )

    part = first_gain.shape[0]
    small_len = 5 * part + up_bias.shape[0]
    small_in = jnp.concatenate(
        [
            first_gain,
            first_shift,
            second_gain,
            second_shift,
            down_bias,
            up_bias,
            jnp.zeros((16 * 128 - small_len,), BF),
        ]
    ).reshape(16, 128)
    joint_in = lax.dynamic_index_in_dim(
        joint_weight.reshape(-1, 3, nh, lc), hi, 2, False
    ).reshape(-1, 3 * lc)
    out_in = lax.dynamic_slice_in_dim(output_weight, hi * lc, lc, 1)
    up_in = lax.dynamic_index_in_dim(
        up_weight.reshape(-1, nd, nh, sub), hi, 2, False
    ).reshape(-1, nd * sub)
    down_in = lax.dynamic_slice_in_dim(down_weight, hi * sub, sub, 0)
    scal = jnp.concatenate(
        [
            jnp.broadcast_to(in_scale, (1, EMB)),
            jnp.broadcast_to(level, (1, EMB)),
            jnp.zeros((6, EMB), F32),
        ]
    )
    blocks = [small_in, input_weight, joint_in, out_in, up_in, down_in]
    scaled, seq_gain, cot, small, in_w, joint_w, out_w, up_w, down_w = link(
        gather_body,
        ident=1,
        outs=[
            ((nh, rows, EMB), BF),
            ((16, EMB), F32),
            ((nh, rows, D), BF),
            ((nd, 16, 128), BF),
            ((nd,) + input_weight.shape, BF),
            ((nd,) + joint_in.shape, BF),
            ((nh, nd) + out_in.shape, BF),
            ((nd,) + up_in.shape, BF),
            ((nd,) + down_in.shape, BF),
        ],
        ins=[parts, noise_input, scal, cotangent] + blocks,
        scratch=[pltpu.VMEM((nd, rows + 16, EMB), BF)],
        sems=8 * nd + 6 * nh,
    )
    scaled_own = lax.dynamic_index_in_dim(scaled, hi, 0, False)
    scaled, cot = scaled.reshape(group, EMB), cot.reshape(group, D)
    seq_gain = seq_gain[: D // EMB].reshape(1, D)
    small = small.reshape(nd, -1)
    gain1, shift1, gain2, shift2, bias_down = [
        small[:, i * part : (i + 1) * part].reshape(1, D).astype(F32) for i in range(5)
    ]
    bias_up = small[:, 5 * part : small_len].reshape(nd, nh, sub)
    bias_up = lax.dynamic_index_in_dim(bias_up, hi, 1, False).reshape(1, -1).astype(F32)
    in_w, joint_w = in_w.reshape(EMB, D), joint_w.reshape(D, 3 * lc)
    out_w = out_w.reshape(nh, D, lc).transpose(1, 0, 2).reshape(D, D)
    up_w, down_w = up_w.reshape(D, nd * sub), down_w.reshape(nd * sub, D)

    def head_all(x, ident):
        (y,) = link(
            head_gather_body,
            ident=ident,
            outs=[((nh,) + x.shape, x.dtype)],
            ins=[x],
            sems=2 * nh,
        )
        return y

    def head_sum(xs, ident):
        n = len(xs)
        shape = (rows, D)
        scratch = [pltpu.VMEM((nh // 2,) + shape, BF)] * (3 * n)
        return link(
            lambda net, *refs: head_reduce_body(net, n, *refs),
            ident=ident,
            outs=[(shape, F32)] * n,
            ins=[x.reshape((nh,) + shape) for x in xs],
            scratch=scratch,
            sems=2 * nh * n,
        )

    stream_in = mm(scaled, in_w)
    hat1, inv1 = norm_parts(stream_in)
    normed1 = (hat1 * gain1 + shift1).astype(BF)
    joint = mm(normed1, joint_w)
    q = rotate(joint[:, :lc], cosine, sine).astype(BF).reshape(group, lh, HSIZE)
    k = rotate(joint[:, lc : 2 * lc], cosine, sine).astype(BF).reshape(group, lh, HSIZE)
    v = joint[:, 2 * lc :].astype(BF).reshape(group, lh, HSIZE)
    allowed = jnp.logical_or(
        jnp.logical_and(live[:, None], live[None, :]), slot[:, None] == slot[None, :]
    )
    scores = jnp.einsum("qhd,khd->hqk", q, k, preferred_element_type=F32) * HSIZE**-0.5
    scores = jnp.where(allowed[None], scores, MASKED)
    exps = jnp.exp(scores - jnp.max(scores, axis=-1, keepdims=True))
    probs = exps / jnp.sum(exps, axis=-1, keepdims=True)
    probs_low = probs.astype(BF)
    attended_own = jnp.einsum(
        "hqk,khd->qhd", probs_low, v, preferred_element_type=F32
    ).astype(BF).reshape(group, lc)
    attended = head_all(attended_own, 2).transpose(1, 0, 2).reshape(group, D)
    stream_mid = stream_in + mm(attended, out_w)
    hat2, inv2 = norm_parts(stream_mid)
    normed2 = (hat2 * gain2 + shift2).astype(BF)
    up_act = mm(normed2, up_w) + bias_up
    gelu_val, gelu_pull = jax.vjp(lambda t: jax.nn.gelu(t, approximate=False), up_act)
    gelu_out = gelu_val.astype(BF)
    ffn_part = mm(gelu_out, down_w).astype(BF)
    grad_stream = cot.astype(F32) * (livef[:, None] * seq_gain)
    grad_branch = grad_stream.astype(BF)
    down_grad = mm(gelu_out, grad_branch, ((0,), (0,)))
    (grad_up,) = gelu_pull(mm(grad_branch, down_w, ((1,), (1,))))
    up_vec = jnp.sum(grad_up, axis=0)
    grad_up_low = grad_up.astype(BF)
    up_grad = mm(normed2, grad_up_low, ((0,), (0,)))
    g2, ffn_own = head_sum([mm(grad_up_low, up_w, ((1,), (1,))).astype(BF), ffn_part], 3)
    stream_out = own(stream_mid) + ffn_own + bias_down
    scale_own = own(livef)[:, None] * seq_gain
    layer_out = scale_own * stream_out
    back2, gain2_p, shift2_p = norm_back(g2, own(hat2), own(inv2), gain2)
    grad_stream_own = cotangent.astype(F32) * scale_own
    grad_mid = grad_stream_own + back2
    grad_mixed_own = grad_mid.astype(BF)
    grad_mixed = head_all(grad_mixed_own, 4).reshape(group, D)
    out_rows = lax.dynamic_slice_in_dim(out_w, hi * lc, lc, 0)
    grad_heads = mm(grad_mixed, out_rows, ((1,), (1,))).astype(BF).reshape(group, lh, HSIZE)
    grad_mixed_cols = lax.dynamic_slice_in_dim(grad_mixed, hi * lc, lc, 1)
    out_grad = mm(attended, grad_mixed_cols, ((0,), (0,)))
    grad_v = jnp.einsum(
        "hqk,qhd->khd", probs_low, grad_heads, preferred_element_type=F32
    ).astype(BF)
    grad_probs = jnp.einsum("qhd,khd->hqk", grad_heads, v, preferred_element_type=F32)
    grad_scores = (
        probs * (grad_probs - jnp.sum(probs * grad_probs, axis=-1, keepdims=True))
    ).astype(BF)
    grad_q = jnp.einsum("hqk,khd->qhd", grad_scores, k, preferred_element_type=F32)
    grad_k = jnp.einsum("hqk,qhd->khd", grad_scores, q, preferred_element_type=F32)
    grad_q = (grad_q * HSIZE**-0.5).astype(BF).astype(F32).reshape(group, lc)
    grad_k = (grad_k * HSIZE**-0.5).astype(BF).astype(F32).reshape(group, lc)
    grad_joint = jnp.concatenate(
        [
            rotate(grad_q, cosine, -sine).astype(BF),
            rotate(grad_k, cosine, -sine).astype(BF),
            grad_v.reshape(group, lc),
        ],
        axis=1,
    )
    joint_grad = mm(normed1, grad_joint, ((0,), (0,)))
    (g1,) = head_sum([mm(grad_joint, joint_w, ((1,), (1,))).astype(BF)], 5)
    back1, gain1_p, shift1_p = norm_back(g1, own(hat1), own(inv1), gain1)
    grad_in_low = (grad_mid + back1).astype(BF)
    input_grad = mm(scaled_own, grad_in_low, ((0,), (0,)))
    grad_scaled = mm(grad_in_low, in_w, ((1,), (1,)))
    noise_grad = (in_scale * level) * grad_scaled
    seq_time = jnp.sum(cotangent.astype(F32) * own(livef)[:, None] * stream_out, axis=0)

    def lanes(x):
        x = x.reshape(nd, 1, -1)
        return jnp.pad(x, ((0, 0), (0, 0), (0, 128 - x.shape[2])))

    dvec = jnp.sum(grad_stream_own, axis=0)
    vecs = [lanes(v) for v in (gain1_p, shift1_p, gain2_p, shift2_p, dvec, up_vec)]
    vecs = jnp.concatenate(vecs + [jnp.zeros((nd, 2, 128), F32)], axis=1)
    terms = [
        down_grad.astype(BF).reshape(nd, sub, D),
        up_grad.astype(BF).reshape(nd, -1, nd * sub),
        out_grad.astype(BF).reshape(nd, -1, lc),
        joint_grad.astype(BF).reshape(nd, -1, 3 * lc),
        input_grad.astype(BF).reshape(nd, -1, D),
        vecs,
    ]
    n = len(terms)
    grad_embed = (in_scale * grad_scaled).astype(BF)
    seq_block = seq_time.reshape(8, 128)
    half = nd // 2
    rings = [pltpu.VMEM((half,) + t.shape[1:], t.dtype) for t in terms]
    *totals, embs, seqs = link(
        lambda net, *refs: final_body(net, n, *refs),
        ident=6,
        outs=[((nh,) + t.shape[1:], t.dtype) for t in terms]
        + [((nh, nd, rows, EMB), BF), ((nh, nd, 8, 128), F32)],
        ins=terms + [grad_embed, seq_block],
        scratch=rings * 2,
        sems=(n + 2) * (nd + 2 * nh),
    )
    down_t, up_t, out_t, joint_t, input_t, vec_t = totals
    ids_all = ints_all[:, :, 0].reshape(-1)
    spread = (vocab_iota[:, None] == ids_all[None, :]).astype(BF)
    table_sum = mm(spread, embs.reshape(-1, EMB))
    table_grad = table_inv * table_sum - table_f * (
        table_inv * table_inv * table_inv
    ) * jnp.mean(table_sum * table_f, axis=1, keepdims=True)
    down_final = down_t.reshape(nh * sub, D).astype(F32)
    up_final = (
        up_t.reshape(nh, -1, nd, sub).transpose(1, 2, 0, 3).reshape(-1, FF).astype(F32)
    )
    out_final = out_t.transpose(1, 0, 2).reshape(-1, D).astype(F32)
    joint_final = (
        joint_t.reshape(nh, -1, 3, lc).transpose(1, 2, 0, 3).reshape(-1, 3 * D).astype(F32)
    )
    input_final = jnp.sum(input_t.astype(F32), axis=0)
    vec_sum = jnp.sum(vec_t[:, :5, :part], axis=0)
    mine = [vec_sum[i] for i in range(5)]
    up_vec = vec_t[:, 5, :sub].reshape(-1)
    time_grad = lax.dot_general(
        time_pick.astype(F32),
        jnp.sum(seqs, axis=0).reshape(nd, D),
        (((0,), (0,)), ((), ())),
        precision=lax.Precision.HIGHEST,
        preferred_element_type=F32,
    )
    return (
        layer_out,
        noise_grad,
        table_grad,
        input_final,
        mine[0],
        mine[1],
        joint_final,
        out_final,
        mine[2],
        mine[3],
        up_final,
        up_vec,
        down_final,
        mine[4],
        time_grad,
    )


def solution(mesh):
    both, dp = P(("dp", "head")), P("dp")
    in_specs = (both, dp, dp, dp, both) + (dp,) * 13 + (both,)
    out_specs = (both, both) + (dp,) * 13
    return jax.shard_map(
        per_device, mesh=mesh, in_specs=in_specs, out_specs=out_specs, check_vma=False
    )
```

```python
import functools
import math

import jax
import jax.numpy as jnp
from jax import lax
from jax.experimental import pallas as pl
from jax.experimental.pallas import tpu as pltpu
from jax.sharding import PartitionSpec as P

D = 1024
HEADS = 16
HSIZE = 64
FF = 4096
EMB = 256
VOCAB = 32000
TIMES = 256
SIG_LO = 0.5
SIG_HI = 4.0
EPS = 1e-05
ROT_BASE = 10000.0
MASKED = -1e30

BF = jnp.bfloat16
F32 = jnp.float32


def mm(a, b, dims=((1,), (0,))):
    return lax.dot_general(a, b, (dims, ((), ())), preferred_element_type=F32)


def rotate(values, cosine, sine):
    half = HSIZE // 2
    v = values.reshape(values.shape[0], -1, HSIZE)
    a, b = v[..., :half], v[..., half:]
    out = jnp.concatenate(
        [a * cosine - b * sine, b * cosine + a * sine], axis=-1
    )
    return out.reshape(values.shape)


def norm_parts(values):
    center = values - jnp.mean(values, axis=-1, keepdims=True)
    inv = lax.rsqrt(jnp.mean(center * center, axis=-1, keepdims=True) + EPS)
    return center * inv, inv


def norm_back(grad, hat, inv, gain):
    e = grad * gain
    back = inv * (
        e
        - jnp.mean(e, axis=-1, keepdims=True)
        - hat * jnp.mean(e * hat, axis=-1, keepdims=True)
    )
    return back, jnp.sum(grad * hat, axis=0), jnp.sum(grad, axis=0)


MESH = pl.DeviceIdType.MESH
VM = pl.BlockSpec(memory_space=pltpu.VMEM)
HB = pl.BlockSpec(memory_space=pl.ANY)


class Net:
    def __init__(self, nd, nh, sends, recvs, locals_=None):
        self.nd, self.nh, self.nx = nd, nh, nh // 2
        self.sends, self.recvs, self.count = sends, recvs, 0
        self.d, self.h = lax.axis_index("dp"), lax.axis_index("head")
        self.x, self.c = self.h // 2, self.h % 2
        y = self.d % 2
        z = self.d // 2
        self.p = z + y * (nd - 1 - 2 * z)
        self.pending = []
        self.locals, self.loaded = locals_, 0

    def at(self, p):
        p = (p + 2 * self.nd) % self.nd
        y = p // (self.nd // 2)
        z = p + y * (self.nd - 1 - 2 * p)
        return z * 2 + y

    def other_chip(self, k):
        return ((self.x + k) % self.nx) * 2 + self.c

    def partner(self):
        return self.x * 2 + 1 - self.c

    def barrier(self, ring=False, dp_all=False, head=False):
        sem = pltpu.get_barrier_semaphore()
        total = 0
        peers = []
        if dp_all:
            peers += [{"dp": (self.d + k) % self.nd} for k in range(1, self.nd)]
        elif ring:
            peers += [{"dp": self.at(self.p + 1)}, {"dp": self.at(self.p - 1)}]
        if head:
            peers += [{"head": self.partner()}]
            peers += [{"head": self.other_chip(k)} for k in range(1, self.nx)]
        for peer in peers:
            pl.semaphore_signal(sem, inc=1, device_id=peer, device_id_type=MESH)
            total += 1
        pl.semaphore_wait(sem, total)

    def send(self, source, target, peer, slot):
        copy = pltpu.make_async_remote_copy(
            src_ref=source,
            dst_ref=target,
            send_sem=self.sends.at[slot],
            recv_sem=self.recvs.at[slot],
            device_id=peer,
            device_id_type=MESH,
        )
        copy.start()
        self.pending.append(copy)
        return copy

    def load(self, source, target):
        copy = pltpu.make_async_copy(source, target, self.locals.at[self.loaded])
        self.loaded += 1
        copy.start()
        return copy

    def slots(self, n):
        first = self.count
        self.count += n
        return first

    def finish(self):
        for copy in self.pending:
            copy.wait_send()


def run(*streams):
    live = list(streams)
    while live:
        for stream in list(live):
            if next(stream, "end") == "end":
                live.remove(stream)


def halves(ref):
    n, w = ref.shape[-2], ref.shape[-1]
    if n % 32 == 0:
        return ref.at[pl.ds(0, n // 2)], ref.at[pl.ds(n // 2, n // 2)]
    if w % 256 == 0:
        return ref.at[:, pl.ds(0, w // 2)], ref.at[:, pl.ds(w // 2, w // 2)]
    return ref, None


def ring_gather(net, buf, view=None):
    view = view or (lambda i: buf.at[i])
    half = net.nd // 2
    first = net.slots(2 * half)
    right, left = {"dp": net.at(net.p + 1)}, {"dp": net.at(net.p - 1)}
    came = []
    for s in range(half):
        for copy in came:
            copy.wait_recv()
        onward, back = view(net.at(net.p - s)), view(net.at(net.p + s))
        if s == half - 1:
            onward, back = halves(onward)[0], halves(back)[1]
        came = [net.send(onward, onward, right, first + 2 * s)]
        if back is not None:
            came.append(net.send(back, back, left, first + 2 * s + 1))
        yield
    for copy in came:
        copy.wait_recv()


def add_into(ref, other):
    ref[...] = (ref[...].astype(F32) + other[...].astype(F32)).astype(ref.dtype)


def ring_reduce(net, terms, fwd, bwd, out):
    half = net.nd // 2
    first = net.slots(2 * half)
    right, left = {"dp": net.at(net.p + 1)}, {"dp": net.at(net.p - 1)}
    a, b = halves(terms.at[net.at(net.p + half)])
    ta, tb = halves(fwd.at[0])[0], halves(bwd.at[0])[1]
    came = [net.send(a, ta, right, first)]
    if b is not None:
        came.append(net.send(b, tb, left, first + 1))
    yield
    for s in range(1, half):
        for copy in came:
            copy.wait_recv()
        own_f, own_b = terms.at[net.at(net.p + half - s)], terms.at[net.at(net.p - half + s)]
        if s == 1:
            (of, of2), (ob2, ob) = halves(own_f), halves(own_b)
            (ff, ff2), (bb2, bb) = halves(fwd.at[0]), halves(bwd.at[0])
            add_into(ff, of)
            if of2 is not None:
                ff2[...] = of2[...]
                add_into(bb, ob)
                bb2[...] = ob2[...]
            else:
                bwd[0] = own_b[...]
        else:
            add_into(fwd.at[s - 1], own_f)
            add_into(bwd.at[s - 1], own_b)
        came = [
            net.send(fwd.at[s - 1], fwd.at[s], right, first + 2 * s),
            net.send(bwd.at[s - 1], bwd.at[s], left, first + 2 * s + 1),
        ]
        yield
    for copy in came:
        copy.wait_recv()
    total = fwd[half - 1].astype(F32) + bwd[half - 1].astype(F32)
    out[...] = (total + terms[net.d].astype(F32)).astype(out.dtype)


def head_gather(net, buf, view=None):
    view = view or (lambda i: buf.at[i])
    nx = net.nx
    first = net.slots(2 * nx)
    mate = {"head": net.partner()}
    own = view(net.h)
    far = [
        net.send(own, own, {"head": net.other_chip(k)}, first + k) for k in range(1, nx)
    ]
    near = [net.send(own, own, mate, first)]
    yield
    for k in range(1, nx):
        far[k - 1].wait_recv()
        block = view(net.other_chip(nx - k))
        near.append(net.send(block, block, mate, first + nx + k))
    yield
    for copy in near:
        copy.wait_recv()


def head_reduce(net, terms, mine, sums, theirs, out):
    nx = net.nx
    first = net.slots(2 * nx)
    mate = {"head": net.partner()}
    order = list(range(1, nx)) + [0]
    near = {}
    for k in order:
        x = (net.x + k) % nx
        near[k] = net.send(terms.at[x * 2 + 1 - net.c], mine.at[x], mate, first + k)
    yield
    far = []
    for k in order:
        x = (net.x + k) % nx
        near[k].wait_recv()
        if k:
            sums[k] = (
                terms[x * 2 + net.c].astype(F32) + mine[x].astype(F32)
            ).astype(sums.dtype)
            peer = {"head": x * 2 + net.c}
            far.append(net.send(sums.at[k], theirs.at[net.x], peer, first + nx + k))
    yield
    total = terms[net.h].astype(F32) + mine[net.x].astype(F32)
    for k in range(1, nx):
        far[k - 1].wait_recv()
        total = total + theirs[(net.x + nx - k) % nx].astype(F32)
    out[...] = total.astype(out.dtype)


def dp_exchange(net, parts, slots):
    nd = net.nd
    first = net.slots(nd)
    came = [
        net.send(
            parts.at[(net.d + k) % nd],
            slots.at[net.d],
            {"dp": (net.d + k) % nd},
            first + k,
        )
        for k in range(1, nd)
    ]
    yield
    for copy in came:
        copy.wait_recv()


def call(body, nd, nh, ident, outs, ins, scratch=(), sems=8, specs=None, out_specs=None):
    def kernel(*refs):
        net = Net(nd, nh, refs[-2], refs[-1])
        body(net, *refs[:-2])
        net.finish()

    return pl.pallas_call(
        kernel,
        out_shape=[jax.ShapeDtypeStruct(*o) for o in outs],
        in_specs=specs or [VM] * len(ins),
        out_specs=out_specs or [VM] * len(outs),
        scratch_shapes=list(scratch)
        + [pltpu.SemaphoreType.DMA((sems,)), pltpu.SemaphoreType.DMA((sems,))],
        compiler_params=pltpu.CompilerParams(
            collective_id=ident, has_side_effects=True
        ),
    )(*ins)


def head_gather_body(net, own, out):
    out[net.h] = own[...]
    net.barrier(head=True)
    run(head_gather(net, out))


def head_reduce_body(net, count, *refs):
    terms, outs = refs[:count], refs[count : 2 * count]
    mine, sums, theirs = [refs[(2 + i) * count : (3 + i) * count] for i in range(3)]
    net.barrier(head=True)
    run(
        *[
            head_reduce(net, terms[i], mine[i], sums[i], theirs[i], outs[i])
            for i in range(count)
        ]
    )


def final_body(net, count, *refs):
    terms = refs[:count]
    emb_in, seq_in = refs[count : count + 2]
    outs = refs[count + 2 : 2 * count + 2]
    emb, seq = refs[2 * count + 2 : 2 * count + 4]
    fwd = refs[2 * count + 4 : 3 * count + 4]
    bwd = refs[3 * count + 4 : 4 * count + 4]
    h, d = net.h, net.d
    emb[h, d] = emb_in[...]
    seq[h, d] = seq_in[...]
    net.barrier(ring=True, head=True)

    def both(ref):
        yield from ring_gather(net, ref.at[h])
        yield from head_gather(net, ref)

    def total(i):
        yield from ring_reduce(net, terms[i], fwd[i], bwd[i], outs[i].at[h])
        yield from head_gather(net, outs[i])

    run(both(emb), both(seq), *[total(i) for i in range(count)])


class Bag:
    def __init__(self, names, refs):
        for name, ref in zip(names, refs, strict=True):
            setattr(self, name, ref)


class Pump:
    def __init__(self, groups):
        self.live = [(begin, stream) for begin, streams in groups for stream in streams]
        self.round = 0

    def __call__(self, times=1):
        for _ in range(times):
            for item in list(self.live):
                if item[0] <= self.round and next(item[1], "end") == "end":
                    self.live.remove(item)
            self.round += 1

    def drain(self):
        while self.live:
            self()


def ring_views(buf, parts):
    width = buf.shape[-1] // parts
    return [
        (lambda i, n=n: buf.at[i, :, pl.ds(n * width, width)]) for n in range(parts)
    ]


def flat_rows(net, small, first, width, total):
    stride = small.shape[1]
    lane = lax.broadcasted_iota(jnp.int32, (128, total), 1)
    spread = (lane % width == lax.broadcasted_iota(jnp.int32, (128, total), 0)).astype(BF)
    rows = small[...].reshape(net.nd * stride, 128)
    wide = mm(rows, spread)
    lane = lax.broadcasted_iota(jnp.int32, wide.shape, 1)
    row = lax.broadcasted_iota(jnp.int32, wide.shape, 0)
    return [
        jnp.sum(
            jnp.where(row == lane // width * stride + place, wide, 0.0), axis=0, keepdims=True
        )
        for place in first
    ]


def join_rows(ref):
    n, rows, width = ref.shape
    if rows % 16 == 0:
        return ref[...].reshape(n * rows, width)
    return jnp.concatenate([ref[i].astype(F32) for i in range(n)], axis=0).astype(ref.dtype)


def swap_halves(value):
    half = HSIZE // 2
    lane = lax.broadcasted_iota(jnp.int32, value.shape, 1)
    down = pltpu.roll(value, value.shape[1] - half, 1)
    up = pltpu.roll(value, half, 1)
    return jnp.where(lane % HSIZE < half, down, up)


def live_masks(r, start, count, group):
    off, size = r.offsets[0], r.lengths[0]
    row = lax.broadcasted_iota(jnp.int32, (count, group), 0) + start
    col = lax.broadcasted_iota(jnp.int32, (count, group), 1)
    live_r = jnp.logical_and(row >= off, row < off + size)
    live_c = jnp.logical_and(col >= off, col < off + size)
    return jnp.logical_or(jnp.logical_and(live_r, live_c), row == col)


def forward_body(net, r, up_sliced):
    nd, nh, d, h = net.nd, net.nh, net.d, net.h
    rows = r.noise.shape[0]
    group = rows * nh
    chunks = group // 128
    lc = r.joint.shape[2] // 3
    nblk = lc // 128
    sub = r.down.shape[1]
    ff = nd * sub
    vrows, trows = r.table.shape[0], r.time_gain.shape[0]
    multiple = pl.multiple_of

    table = net.load(r.embed_table, r.table)
    loads = [net.load(r.cotangent, r.cots.at[h]), net.load(r.input_weight, r.in_w.at[d])]
    for j in range(3):
        cols = pl.ds(multiple(j * D + h * lc, 128), lc)
        loads.append(
            net.load(r.joint_weight.at[:, cols], r.joint.at[d, :, pl.ds(j * lc, lc)])
        )
    cols = pl.ds(multiple(h * lc, 128), lc)
    loads.append(net.load(r.output_weight.at[:, cols], r.out.at[h, d]))
    if up_sliced:
        loads.append(net.load(r.up_weight, r.up.at[d]))
    else:
        for q in range(nd):
            cols = pl.ds(multiple((q * nh + h) * sub, 128), sub)
            loads.append(
                net.load(r.up_weight.at[:, cols], r.up.at[d, :, pl.ds(q * sub, sub)])
            )
    place = pl.ds(multiple(h * sub, 16), sub)
    loads.append(net.load(r.down_weight.at[place], r.down.at[d]))
    r.small[d] = r.small_in[...]
    r.ints[h, d] = r.ints_in[...]
    net.barrier(dp_all=True, head=True)

    first = net.slots(nd)
    own = r.ints.at[h, d]
    ids_came = [
        net.send(own, own, {"dp": (d + k) % nd}, first + k) for k in range(1, nd)
    ]
    for copy in loads:
        copy.wait()

    def outer():
        yield from ring_gather(net, r.out.at[h])
        yield from head_gather(net, r.out)

    half = nd // 2
    pump = Pump(
        [
            (0, [ring_gather(net, r.in_w), ring_gather(net, r.small)]),
            (0, [ring_gather(net, r.joint), outer(), head_gather(net, r.cots)]),
            (half - 1, [ring_gather(net, r.up, v) for v in ring_views(r.up, 2)]),
            (2 * half - 2, [ring_gather(net, r.down, v) for v in ring_views(r.down, 2)]),
        ]
    )
    pump()

    table.wait()
    step = 400 if vrows % 400 == 0 else vrows

    def unit(i, carry):
        at = pl.ds(multiple(i * step, 8), step)
        x = r.table[at].astype(F32)
        inv = lax.rsqrt(jnp.mean(x * x, axis=1, keepdims=True) + EPS)
        r.table[at] = (x * inv).astype(BF)
        return carry

    lax.fori_loop(0, vrows // step, unit, 0)
    for copy in ids_came:
        copy.wait_recv()
    ids_far = head_gather(net, r.ints)
    next(ids_far)

    first_e, first_t = net.slots(nd), net.slots(nd)

    def peer_copy(k, sent, came, base):
        return pltpu.make_async_remote_copy(
            src_ref=sent.at[(d + k) % nd],
            dst_ref=came.at[d],
            send_sem=net.sends.at[base + k],
            recv_sem=net.recvs.at[base + k],
            device_id={"dp": (d + k) % nd},
            device_id_type=MESH,
        )

    def look_up(k, carry):
        t = (d + k) % nd
        block = r.ints[h, t]
        ids = jnp.transpose(block)[:, 0:1]
        vocab = lax.broadcasted_iota(jnp.int32, (rows, vrows), 1) + d * vrows
        pick = jnp.where(ids == vocab, 1.0, 0.0).astype(BF)
        r.parts[t] = mm(pick, r.table[...]).astype(BF)
        times = lax.broadcasted_iota(jnp.int32, (trows, D), 0) + d * trows
        hit = times == block[1:2, 0:1]
        r.tparts[t] = jnp.sum(
            jnp.where(hit, r.time_gain[...].astype(F32), 0.0), axis=0, keepdims=True
        )

        @pl.when(k > 0)
        def _():
            peer_copy(k, r.parts, r.slots, first_e).start()
            peer_copy(k, r.tparts, r.tslots, first_t).start()

        return carry

    third = nd // 4
    lax.fori_loop(0, third, look_up, 0)
    pump()
    lax.fori_loop(third, 3 * third, look_up, 0)
    pump()
    lax.fori_loop(3 * third, nd, look_up, 0)
    r.slots[d] = r.parts[d]
    r.tslots[d] = r.tparts[d]

    def arrive(k, carry):
        peer_copy(k, r.parts, r.slots, first_e).wait()
        peer_copy(k, r.tparts, r.tslots, first_t).wait()
        return carry

    lax.fori_loop(1, nd, arrive, 0)
    embedded = r.slots[0].astype(F32)
    seq_gain = r.tslots[0]
    for k in range(1, nd):
        embedded = embedded + r.slots[k].astype(F32)
        seq_gain = seq_gain + r.tslots[k]
    value = r.scal[0:1] * (embedded + r.scal[1:2] * r.noise[...].astype(F32))
    r.scaled[h] = value.astype(BF)
    scaled_all = head_gather(net, r.scaled)
    next(scaled_all)
    pump()
    run(ids_far)
    run(scaled_all)
    pump()

    part = D // nd
    for i, v in enumerate(flat_rows(net, r.small, range(5), part, D)):
        r.vecs[i : i + 1] = v
    r.vecs[5:6] = seq_gain
    in_w = join_rows(r.in_w)
    scaled = r.scaled[...].reshape(group, EMB)
    for n in range(D // 256):
        r.stream[:, n * 256 : (n + 1) * 256] = mm(scaled, in_w[:, n * 256 : (n + 1) * 256])

    def norm(gain, shift, target):
        def body(i, carry):
            at = pl.ds(multiple(i * 64, 64), 64)
            hat, _ = norm_parts(r.stream[at])
            target[at] = (hat * r.vecs[gain : gain + 1] + r.vecs[shift : shift + 1]).astype(BF)
            return carry

        lax.fori_loop(0, group // 64, body, 0)

    norm(0, 1, r.normed1)
    r.in_own[...] = r.stream[pl.ds(multiple(h * rows, 128), rows)]
    for j in range(3):
        for b in range(nblk):
            cols = slice(j * lc + b * 128, j * lc + (b + 1) * 128)
            w = r.joint[:, :, cols].reshape(D, 128)
            value = mm(r.normed1[...], w)
            if j < 2:
                value = value * r.cosine[...] + swap_halves(value) * r.sine[...]
            (r.q, r.k, r.v)[j][b] = value.astype(BF)

    att_streams = []
    for b in range(nblk):

        def attend(i, carry, b=b):
            at = pl.ds(multiple(i * 128, 128), 128)
            lane = lax.broadcasted_iota(jnp.int32, (128, 128), 1)
            allowed = live_masks(r, i * 128, 128, group)
            results = []
            for e in range(2):
                mine = lane // HSIZE == e
                q = jnp.where(mine, r.q[b, at], jnp.zeros((), BF))
                scores = mm(q, r.k[b], ((1,), (1,))) * HSIZE**-0.5
                scores = jnp.where(allowed, scores, MASKED)
                exps = jnp.exp(scores - jnp.max(scores, axis=1, keepdims=True))
                probs = (exps / jnp.sum(exps, axis=1, keepdims=True)).astype(BF)
                r.probs[2 * b + e, at] = probs
                results.append(mm(probs, r.v[b]))
            r.att[h, b, at] = jnp.where(lane < HSIZE, results[0], results[1]).astype(BF)
            return carry

        lax.fori_loop(0, chunks, attend, 0)
        stream = head_gather(net, r.att, lambda i, b=b: r.att.at[i, b])
        next(stream)
        for other in att_streams:
            next(other, None)
        att_streams.append(stream)
        pump()
    run(*att_streams)

    attended = jnp.concatenate(
        [r.att[i, b] for i in range(nh) for b in range(nblk)], axis=1
    )
    for i in range(nh):
        cols = slice(i * lc, (i + 1) * lc)
        r.stream[:, cols] = r.stream[:, cols] + mm(attended, r.out[i].reshape(D, lc))
    r.mid_own[...] = r.stream[pl.ds(multiple(h * rows, 128), rows)]
    norm(2, 3, r.normed2)
    pump()
    (bias,) = flat_rows(net, r.small, [5 + h], sub, ff)
    r.bias[...] = bias
    for n in range(ff // 256):
        cols = slice(n * 256, (n + 1) * 256)
        act = mm(r.normed2[...], r.up[:, :, cols].reshape(D, 256)) + r.bias[:, cols]
        cdf = 0.5 * (1.0 + lax.erf(act * (0.5**0.5)))
        pdf = jnp.exp(-0.5 * act * act) * ((2.0 * math.pi) ** -0.5)
        r.gelu[:, cols] = (act * cdf).astype(BF)
        r.dgelu[:, cols] = (cdf + act * pdf).astype(BF)
        if n % 2 == 1:
            pump()
    pump.drain()


def kernel_call(body, nd, nh, ident, ins, outs, scratch, sems):
    names = list(ins) + list(outs) + list(scratch)

    def kernel(*refs):
        net = Net(nd, nh, refs[-3], refs[-2], refs[-1])
        body(net, Bag(names, refs[:-3]))
        net.finish()

    result = pl.pallas_call(
        kernel,
        out_shape=[jax.ShapeDtypeStruct(*o) for o in outs.values()],
        in_specs=[spec for _, spec in ins.values()],
        out_specs=[VM] * len(outs),
        scratch_shapes=[pltpu.VMEM(*s) for s in scratch.values()]
        + [pltpu.SemaphoreType.DMA((sems,))] * 2
        + [pltpu.SemaphoreType.DMA((nd + 16,))],
        compiler_params=pltpu.CompilerParams(
            collective_id=ident, has_side_effects=True, vmem_limit_bytes=64 << 20
        ),
    )(*[x for x, _ in ins.values()])
    return dict(zip(outs, result, strict=True))


def per_device(
    token_ids,
    lengths,
    offsets,
    time_steps,
    noise_input,
    embed_table,
    input_weight,
    first_gain,
    first_shift,
    joint_weight,
    output_weight,
    second_gain,
    second_shift,
    up_weight,
    up_bias,
    down_weight,
    down_bias,
    time_gain,
    cotangent,
):
    nd, nh = lax.axis_size("dp"), lax.axis_size("head")
    di, hi = lax.axis_index("dp"), lax.axis_index("head")
    rows = token_ids.shape[0]
    group = rows * nh
    lh = HEADS // nh
    lc = lh * HSIZE
    sub = FF // (nd * nh)
    vrows = embed_table.shape[0]
    trows = time_gain.shape[0]

    slot = jnp.arange(group, dtype=jnp.int32)
    live = jnp.logical_and(slot >= offsets[0], slot < offsets[0] + lengths[0])
    livef = live.astype(F32)
    position = (slot - offsets[0]).astype(F32)
    level = jnp.exp(
        math.log(SIG_LO)
        + time_steps[0].astype(F32) * (math.log(SIG_HI / SIG_LO) / (TIMES - 1))
    )
    in_scale = lax.rsqrt(1.0 + level * level)
    half_size = HSIZE // 2
    lane = jnp.arange(128, dtype=jnp.int32)
    freqs = jnp.exp(-math.log(ROT_BASE) * (lane % half_size).astype(F32) / half_size)
    angle = position[:, None] * freqs[None, :]
    cos_wide = jnp.cos(angle)
    sin_wide = jnp.where(lane % HSIZE < half_size, -1.0, 1.0) * jnp.sin(angle)
    cosine = cos_wide[:, None, :half_size]
    sine = -sin_wide[:, None, :half_size]

    def own(x):
        return lax.dynamic_slice_in_dim(x, hi * rows, rows, 0)

    link = functools.partial(call, nd=nd, nh=nh)
    ints = jnp.concatenate(
        [
            token_ids[None],
            jnp.broadcast_to(time_steps[:, None], (1, rows)),
            jnp.zeros((6, rows), jnp.int32),
        ]
    )
    part = first_gain.shape[0]
    ff = nd * sub
    nblk = lc // 128

    def place(v, row, count=1):
        v = v.reshape(count, -1)
        return jnp.pad(v, ((row, 16 - row - count), (0, 128 - v.shape[1])))

    small_in = place(up_bias, 5, nh)
    for i, v in enumerate((first_gain, first_shift, second_gain, second_shift, down_bias)):
        small_in = small_in + place(v, i)
    up_sliced = sub % 128 != 0
    up_in = up_weight
    if up_sliced:
        up_in = lax.dynamic_index_in_dim(
            up_weight.reshape(-1, nd, nh, sub), hi, 2, False
        ).reshape(-1, ff)
    scal = jnp.where(
        jnp.arange(8)[:, None] == 0, in_scale, jnp.broadcast_to(level, (8, EMB))
    )
    sm = pl.BlockSpec(memory_space=pltpu.SMEM)
    fw = kernel_call(
        lambda net, r: forward_body(net, r, up_sliced),
        nd,
        nh,
        0,
        ins=dict(
            ints_in=(ints, VM),
            lengths=(lengths, sm),
            offsets=(offsets, sm),
            scal=(scal, VM),
            cosine=(cos_wide, VM),
            sine=(sin_wide, VM),
            noise=(noise_input, VM),
            time_gain=(time_gain, VM),
            small_in=(small_in, VM),
            embed_table=(embed_table, HB),
            cotangent=(cotangent, HB),
            input_weight=(input_weight, HB),
            joint_weight=(joint_weight, HB),
            output_weight=(output_weight, HB),
            up_weight=(up_in, HB),
            down_weight=(down_weight, HB),
        ),
        outs=dict(
            ints=((nh, nd, 8, rows), jnp.int32),
            cots=((nh, rows, D), BF),
            in_w=((nd,) + input_weight.shape, BF),
            joint=((nd, D // nd, 3 * lc), BF),
            out=((nh, nd, D // nd, lc), BF),
            up=((nd, D // nd, ff), BF),
            down=((nd, sub, D), BF),
            vecs=((8, D), F32),
            scaled=((nh, rows, EMB), BF),
            in_own=((rows, D), F32),
            mid_own=((rows, D), F32),
            normed1=((group, D), BF),
            normed2=((group, D), BF),
            q=((nblk, group, 128), BF),
            k=((nblk, group, 128), BF),
            v=((nblk, group, 128), BF),
            probs=((lh, group, group), BF),
            att=((nh, nblk, group, 128), BF),
            gelu=((group, ff), BF),
            dgelu=((group, ff), BF),
        ),
        scratch=dict(
            table=((vrows, EMB), BF),
            small=((nd, 16, 128), BF),
            parts=((nd, rows, EMB), BF),
            slots=((nd, rows, EMB), BF),
            tparts=((nd, 1, D), F32),
            tslots=((nd, 1, D), F32),
            stream=((group, D), F32),
            bias=((1, ff), F32),
        ),
        sems=12 * nd + 8 * nh,
    )
    ints_all = fw["ints"]
    times_all = ints_all[0, :, 1, 0]
    time_iota = jnp.arange(trows, dtype=jnp.int32) + di * trows
    time_pick = (times_all[:, None] == time_iota[None, :]).astype(BF)
    vocab_iota = jnp.arange(vrows, dtype=jnp.int32) + di * vrows
    table_f = embed_table.astype(F32)
    table_inv = lax.rsqrt(jnp.mean(table_f * table_f, axis=1, keepdims=True) + EPS)
    scaled_own = lax.dynamic_index_in_dim(fw["scaled"], hi, 0, False)
    cot = fw["cots"].reshape(group, D)
    gain1, shift1, gain2, shift2, bias_down, seq_gain = [
        fw["vecs"][i : i + 1] for i in range(6)
    ]
    in_w, joint_w = fw["in_w"].reshape(EMB, D), fw["joint"].reshape(D, 3 * lc)
    out_w = fw["out"].reshape(nh, D, lc).transpose(1, 0, 2).reshape(D, D)
    up_w, down_w = fw["up"].reshape(D, ff), fw["down"].reshape(ff, D)

    def head_all(x, ident):
        (y,) = link(
            head_gather_body,
            ident=ident,
            outs=[((nh,) + x.shape, x.dtype)],
            ins=[x],
            sems=2 * nh,
        )
        return y

    def head_sum(xs, ident):
        n = len(xs)
        shape = (rows, D)
        scratch = [pltpu.VMEM((nh // 2,) + shape, BF)] * (3 * n)
        return link(
            lambda net, *refs: head_reduce_body(net, n, *refs),
            ident=ident,
            outs=[(shape, F32)] * n,
            ins=[x.reshape((nh,) + shape) for x in xs],
            scratch=scratch,
            sems=2 * nh * n,
        )

    def heads(x):
        return x.transpose(1, 0, 2).reshape(group, lh, HSIZE)

    q, k, v = heads(fw["q"]), heads(fw["k"]), heads(fw["v"])
    probs_low = fw["probs"]
    probs = probs_low.astype(F32)
    attended = fw["att"].transpose(2, 0, 1, 3).reshape(group, D)
    normed1, normed2, gelu_out = fw["normed1"], fw["normed2"], fw["gelu"]
    hat1, inv1 = norm_parts(fw["in_own"])
    hat2, inv2 = norm_parts(fw["mid_own"])
    ffn_part = mm(gelu_out, down_w).astype(BF)
    scale_own = own(livef)[:, None] * seq_gain
    grad_stream = cot.astype(F32) * (livef[:, None] * seq_gain)
    grad_branch = grad_stream.astype(BF)
    down_grad = mm(gelu_out, grad_branch, ((0,), (0,)))
    grad_up = mm(grad_branch, down_w, ((1,), (1,))) * fw["dgelu"].astype(F32)
    up_vec = jnp.sum(grad_up, axis=0)
    grad_up_low = grad_up.astype(BF)
    up_grad = mm(normed2, grad_up_low, ((0,), (0,)))
    g2, ffn_own = head_sum([mm(grad_up_low, up_w, ((1,), (1,))).astype(BF), ffn_part], 3)
    stream_out = fw["mid_own"] + ffn_own + bias_down
    layer_out = scale_own * stream_out
    back2, gain2_p, shift2_p = norm_back(g2, hat2, inv2, gain2)
    grad_stream_own = cotangent.astype(F32) * scale_own
    grad_mid = grad_stream_own + back2
    grad_mixed_own = grad_mid.astype(BF)
    grad_mixed = head_all(grad_mixed_own, 4).reshape(group, D)
    out_rows = lax.dynamic_slice_in_dim(out_w, hi * lc, lc, 0)
    grad_heads = mm(grad_mixed, out_rows, ((1,), (1,))).astype(BF).reshape(group, lh, HSIZE)
    grad_mixed_cols = lax.dynamic_slice_in_dim(grad_mixed, hi * lc, lc, 1)
    out_grad = mm(attended, grad_mixed_cols, ((0,), (0,)))
    grad_v = jnp.einsum(
        "hqk,qhd->khd", probs_low, grad_heads, preferred_element_type=F32
    ).astype(BF)
    grad_probs = jnp.einsum("qhd,khd->hqk", grad_heads, v, preferred_element_type=F32)
    grad_scores = (
        probs * (grad_probs - jnp.sum(probs * grad_probs, axis=-1, keepdims=True))
    ).astype(BF)
    grad_q = jnp.einsum("hqk,khd->qhd", grad_scores, k, preferred_element_type=F32)
    grad_k = jnp.einsum("hqk,qhd->khd", grad_scores, q, preferred_element_type=F32)
    grad_q = (grad_q * HSIZE**-0.5).astype(BF).astype(F32).reshape(group, lc)
    grad_k = (grad_k * HSIZE**-0.5).astype(BF).astype(F32).reshape(group, lc)
    grad_joint = jnp.concatenate(
        [
            rotate(grad_q, cosine, -sine).astype(BF),
            rotate(grad_k, cosine, -sine).astype(BF),
            grad_v.reshape(group, lc),
        ],
        axis=1,
    )
    joint_grad = mm(normed1, grad_joint, ((0,), (0,)))
    (g1,) = head_sum([mm(grad_joint, joint_w, ((1,), (1,))).astype(BF)], 5)
    back1, gain1_p, shift1_p = norm_back(g1, hat1, inv1, gain1)
    grad_in_low = (grad_mid + back1).astype(BF)
    input_grad = mm(scaled_own, grad_in_low, ((0,), (0,)))
    grad_scaled = mm(grad_in_low, in_w, ((1,), (1,)))
    noise_grad = (in_scale * level) * grad_scaled
    seq_time = jnp.sum(cotangent.astype(F32) * own(livef)[:, None] * stream_out, axis=0)

    def lanes(x):
        x = x.reshape(nd, 1, -1)
        return jnp.pad(x, ((0, 0), (0, 0), (0, 128 - x.shape[2])))

    dvec = jnp.sum(grad_stream_own, axis=0)
    vecs = [lanes(v) for v in (gain1_p, shift1_p, gain2_p, shift2_p, dvec, up_vec)]
    vecs = jnp.concatenate(vecs + [jnp.zeros((nd, 2, 128), F32)], axis=1)
    terms = [
        down_grad.astype(BF).reshape(nd, sub, D),
        up_grad.astype(BF).reshape(nd, -1, nd * sub),
        out_grad.astype(BF).reshape(nd, -1, lc),
        joint_grad.astype(BF).reshape(nd, -1, 3 * lc),
        input_grad.astype(BF).reshape(nd, -1, D),
        vecs,
    ]
    n = len(terms)
    grad_embed = (in_scale * grad_scaled).astype(BF)
    seq_block = seq_time.reshape(8, 128)
    half = nd // 2
    rings = [pltpu.VMEM((half,) + t.shape[1:], t.dtype) for t in terms]
    *totals, embs, seqs = link(
        lambda net, *refs: final_body(net, n, *refs),
        ident=6,
        outs=[((nh,) + t.shape[1:], t.dtype) for t in terms]
        + [((nh, nd, rows, EMB), BF), ((nh, nd, 8, 128), F32)],
        ins=terms + [grad_embed, seq_block],
        scratch=rings * 2,
        sems=(n + 2) * (nd + 2 * nh),
    )
    down_t, up_t, out_t, joint_t, input_t, vec_t = totals
    ids_all = ints_all[:, :, 0].reshape(-1)
    spread = (vocab_iota[:, None] == ids_all[None, :]).astype(BF)
    table_sum = mm(spread, embs.reshape(-1, EMB))
    table_grad = table_inv * table_sum - table_f * (
        table_inv * table_inv * table_inv
    ) * jnp.mean(table_sum * table_f, axis=1, keepdims=True)
    down_final = down_t.reshape(nh * sub, D).astype(F32)
    up_final = (
        up_t.reshape(nh, -1, nd, sub).transpose(1, 2, 0, 3).reshape(-1, FF).astype(F32)
    )
    out_final = out_t.transpose(1, 0, 2).reshape(-1, D).astype(F32)
    joint_final = (
        joint_t.reshape(nh, -1, 3, lc).transpose(1, 2, 0, 3).reshape(-1, 3 * D).astype(F32)
    )
    input_final = jnp.sum(input_t.astype(F32), axis=0)
    vec_sum = jnp.sum(vec_t[:, :5, :part], axis=0)
    mine = [vec_sum[i] for i in range(5)]
    up_vec = vec_t[:, 5, :sub].reshape(-1)
    time_grad = lax.dot_general(
        time_pick.astype(F32),
        jnp.sum(seqs, axis=0).reshape(nd, D),
        (((0,), (0,)), ((), ())),
        precision=lax.Precision.HIGHEST,
        preferred_element_type=F32,
    )
    return (
        layer_out,
        noise_grad,
        table_grad,
        input_final,
        mine[0],
        mine[1],
        joint_final,
        out_final,
        mine[2],
        mine[3],
        up_final,
        up_vec,
        down_final,
        mine[4],
        time_grad,
    )


def solution(mesh):
    both, dp = P(("dp", "head")), P("dp")
    in_specs = (both, dp, dp, dp, both) + (dp,) * 13 + (both,)
    out_specs = (both, both) + (dp,) * 13
    return jax.shard_map(
        per_device, mesh=mesh, in_specs=in_specs, out_specs=out_specs, check_vma=False
    )
```
